32 devices in a mesh: row: 8 (over z, y), col: 4 (over x, core).
Axes of the slice: x: 2, y: 2, z: 4, core: 2. Of those that a mesh axis runs over, the one named last changes fastest.
Arguments:
- eigvec: float32 [32, 8, 128, 1024], P(None, 'row', None, 'col'), may hold values from -6 to 6
- reflectors: float32 [2, 32, 8, 256, 128], P(None, None, 'row', 'col'), may hold values from -6 to 6
- sweep_group: int32 [2, 32, 8], P(None, None, 'row'), may hold values from -1 to 254, as said below
Outputs:
- transformed: float32 [32, 8, 128, 1024], P(None, 'row', None, 'col')
The draws below stay inside these ranges and needn't reach their ends.
Inputs may be any that keep to these rules, and one draw needn't show every extreme that they name: `sweep_group`: -1 where no diamond sits at that diagonal and tile position (tile position l * R + r for entry [d, l, r]); otherwise the diamond's sweep group, at most its tile position. Within one diagonal no two diamonds sit at adjacent tile positions, and none sits at the last tile position 255.
All inputs are finite; a program needn't handle non-finite values.
Results may differ from the reference program's by a relative error of at most 0.0003.
Values sent between devices are 32-bit elements.
A program may use at most 128 MiB of HBM per device.

```python
import jax
import jax.numpy as jnp
from jax import lax

B = 128
DIAG = 2
NT = 256
TILES_DEV = 32
NC = 1024
N_ROW = 8


def draw_sweep_group(key, part):
    first_key = jax.random.fold_in(key, 11)
    second_key = jax.random.fold_in(key, 12)
    bits = jax.random.randint(first_key, (DIAG, NT), 0, 2).astype(jnp.int32)
    earlier = jnp.concatenate([jnp.zeros((DIAG, 1), jnp.int32), bits[:, :-1]], axis=1)
    positions = jnp.broadcast_to(jnp.arange(NT, dtype=jnp.int32)[None, :], (DIAG, NT))
    present = (bits == 1) & (earlier == 0) & (positions < NT - 1)
    groups = jax.random.randint(second_key, (DIAG, NT), 0, positions + 1).astype(jnp.int32)
    result = jnp.where(present, groups, -jnp.ones_like(groups))
    return result.reshape(DIAG, TILES_DEV, NT // TILES_DEV).astype(jnp.int32)


def level_of(key, dims, shards, least, largest):
    def one(dim, shards_of):
        steps = jax.random.uniform(jax.random.fold_in(jax.random.fold_in(key, 6), dim), (shards_of,), jnp.float32, least / len(shards), largest / len(shards))
        return jnp.repeat(jnp.exp(steps), dims[dim] // shards_of).reshape((-1,) + (1,) * (len(dims) - dim - 1))

    factor_of = one(*shards[0])
    for cut in shards[1:]:
        factor_of = factor_of * one(*cut)
    return factor_of


def gaussian(key, shape, deviation, reach, shards=(), kind=jnp.bfloat16):
    values = deviation * jax.random.normal(key, shape, jnp.float32)
    if shards:
        values = values * level_of(key, shape, shards, -0.22, 0.18)
    return jnp.clip(values, -reach, reach).astype(kind)


def setup_inputs(seed: int = 0) -> dict:
    streams_of = jax.random.split(jax.random.key(seed), 4)
    return {
        "eigvec": gaussian(streams_of[0], (TILES_DEV, N_ROW, B, NC), 1.0, 6.0, ((1, 8), (3, 4)), jnp.float32),
        "reflectors": gaussian(streams_of[1], (DIAG, TILES_DEV, N_ROW, 2 * B, B), 1.0, 6.0, ((2, 8), (3, 4)), jnp.float32),
        "sweep_group": draw_sweep_group(jax.random.fold_in(streams_of[3], 71), 0),
    }


highest_mode = lax.Precision.HIGHEST


def masked_vectors(panels):
    depth_rows = panels.shape[-2]
    band_width = panels.shape[-1]
    row_iota = lax.broadcasted_iota(jnp.int32, (depth_rows, band_width), 0)
    col_iota = lax.broadcasted_iota(jnp.int32, (depth_rows, band_width), 1)
    inside = (row_iota >= col_iota + 1) & (row_iota <= col_iota + band_width)
    leading = row_iota == col_iota + 1
    kept = jnp.where(inside, panels, jnp.zeros_like(panels))
    return jnp.where(leading, jnp.ones_like(panels), kept)


def inverse_factor(vectors):
    band_width = vectors.shape[-1]
    gram_matrix = jnp.einsum("...ji,...jk->...ik", vectors, vectors, precision=highest_mode)
    diagonal_part = jnp.diagonal(gram_matrix, axis1=-2, axis2=-1)
    strict_upper = jnp.triu(gram_matrix, 1)
    return strict_upper + jnp.eye(band_width, dtype=vectors.dtype) * (0.5 * diagonal_part[..., None, :])


def invert_upper(factor):
    band_width = factor.shape[-1]
    row_iota = lax.broadcasted_iota(jnp.int32, (band_width, band_width), 0)
    col_iota = lax.broadcasted_iota(jnp.int32, (band_width, band_width), 1)
    diagonal_part = jnp.diagonal(factor, axis1=-2, axis2=-1)
    eye_matrix = (row_iota == col_iota).astype(factor.dtype)
    inverse = eye_matrix * (1.0 / diagonal_part)[..., None, :]
    block = 1
    while block < band_width:
        coupling = ((row_iota // block) != (col_iota // block)) & ((row_iota // (2 * block)) == (col_iota // (2 * block)))
        upper_part = jnp.where(coupling, factor, jnp.zeros_like(factor))
        middle = jnp.einsum("...ij,...jk->...ik", upper_part, inverse, precision=highest_mode)
        inverse = inverse - jnp.einsum("...ij,...jk->...ik", inverse, middle, precision=highest_mode)
        block = block * 2
    return inverse


def reflect(stacked, vectors, factor):
    weights = jnp.einsum("...ji,...jc->...ic", vectors, stacked, precision=highest_mode)
    solved = jnp.einsum("...ik,...kc->...ic", invert_upper(factor), weights, precision=highest_mode)
    return stacked - jnp.einsum("...ji,...ic->...jc", vectors, solved, precision=highest_mode)


def apply_one(item):
    stacked, panels, flag = item
    vectors = masked_vectors(panels)
    factor = inverse_factor(vectors)
    updated = reflect(stacked, vectors, factor)
    return jnp.where(flag >= 0, updated, stacked)


def reference(eigvec, reflectors, sweep_group):
    tiles_dev = eigvec.shape[0]
    cycle_size = eigvec.shape[1]
    band = eigvec.shape[2]
    columns = eigvec.shape[3]
    total = tiles_dev * cycle_size
    diagonals = reflectors.shape[0]
    current = eigvec.reshape(total, band, columns)
    panels_all = reflectors.reshape(diagonals, total, 2 * band, band)
    flags_all = sweep_group.reshape(diagonals, total)
    for diagonal in range(diagonals):
        stacked = current.reshape(total // 2, 2 * band, columns)
        updated = lax.map(apply_one, (stacked, panels_all[diagonal, 0::2], flags_all[diagonal, 0::2]))
        current = updated.reshape(total, band, columns)
        inner = current[1:total - 1].reshape(total // 2 - 1, 2 * band, columns)
        updated = lax.map(apply_one, (inner, panels_all[diagonal, 1:total - 1:2], flags_all[diagonal, 1:total - 1:2]))
        current = jnp.concatenate([current[:1], updated.reshape(total - 2, band, columns), current[total - 1:]], axis=0)
    return current.reshape(tiles_dev, cycle_size, band, columns)
```

```python
import functools

import jax
import jax.numpy as jnp
from jax import lax
from jax.experimental import pallas as pl
from jax.experimental.pallas import tpu as pltpu
from jax.sharding import PartitionSpec as P

SLOT_SIZES = (8, 10, 12, 14, 16)
GROUP = 2


def split(x):
    high = x.astype(jnp.bfloat16)
    return high, (x - high.astype(jnp.float32)).astype(jnp.bfloat16)


def dot(a, b):
    return jnp.dot(a, b, preferred_element_type=jnp.float32)


def dot3(a, b):
    return dot(a[1], b[0]) + dot(a[0], b[1]) + dot(a[0], b[0])


def gather_kernel(slots, own, behind, panels, tiles, picked, sent, sems):
    diagonals = panels.shape[0]

    def panel_copy(d, k):
        return pltpu.make_async_copy(
            panels.at[d, own[d, k]], picked.at[d, k], sems.at[d * slots + k]
        )

    def tile_copy(k):
        return pltpu.make_async_copy(
            tiles.at[behind[0, k]], sent.at[k], sems.at[diagonals * slots + k]
        )

    for k in range(slots):
        tile_copy(k).start()
    for d in range(diagonals):
        for k in range(slots):
            panel_copy(d, k).start()
    for k in range(slots):
        tile_copy(k).wait()
    for d in range(diagonals):
        for k in range(slots):
            panel_copy(d, k).wait()


def gather(slots, own, behind, panels, tiles):
    diagonals = panels.shape[0]
    any_spec = pl.BlockSpec(memory_space=pl.ANY)
    return pl.pallas_call(
        functools.partial(gather_kernel, slots),
        grid_spec=pltpu.PrefetchScalarGridSpec(
            num_scalar_prefetch=2,
            grid=(1,),
            in_specs=[any_spec, any_spec],
            out_specs=[any_spec, any_spec],
            scratch_shapes=[pltpu.SemaphoreType.DMA(((diagonals + 1) * slots,))],
        ),
        out_shape=[
            jax.ShapeDtypeStruct((diagonals, slots) + panels.shape[2:], panels.dtype),
            jax.ShapeDtypeStruct((slots,) + tiles.shape[1:], tiles.dtype),
        ],
        name="gather",
    )(own, behind, panels, tiles)


def scatter_kernel(slots, diagonal, more, behind, counts, tiles, returned, out, *rest):
    sems = rest[-1]

    def put(k):
        return pltpu.make_async_copy(
            returned.at[k], out.at[behind[diagonal, k]], sems.at[k]
        )

    for k in range(slots):
        @pl.when(k < counts[1, diagonal])
        def _():
            put(k).start()
    for k in range(slots):
        @pl.when(k < counts[1, diagonal])
        def _():
            put(k).wait()
    if more:
        sent = rest[0]

        def take(k):
            return pltpu.make_async_copy(
                out.at[behind[diagonal + 1, k]], sent.at[k], sems.at[slots + k]
            )

        for k in range(slots):
            take(k).start()
        for k in range(slots):
            take(k).wait()


def scatter(slots, diagonal, more, behind, counts, tiles, returned):
    any_spec = pl.BlockSpec(memory_space=pl.ANY)
    shapes = [jax.ShapeDtypeStruct(tiles.shape, tiles.dtype)]
    if more:
        shapes.append(jax.ShapeDtypeStruct(returned.shape, returned.dtype))
    return pl.pallas_call(
        functools.partial(scatter_kernel, slots, diagonal, more),
        grid_spec=pltpu.PrefetchScalarGridSpec(
            num_scalar_prefetch=2,
            grid=(1,),
            in_specs=[any_spec, any_spec],
            out_specs=[any_spec] * len(shapes),
            scratch_shapes=[pltpu.SemaphoreType.DMA((2 * slots,))],
        ),
        out_shape=shapes,
        input_output_aliases={2: 0},
        name="scatter",
    )(behind, counts, tiles, returned)


def factor_kernel(pieces_count, col_ref, *refs):
    pieces = refs[:pieces_count]
    vh_ref, vl_ref, yh_ref, yl_ref = refs[pieces_count:]
    me = col_ref[0]
    group = pieces[0].shape[1]
    band = pieces[0].shape[-1]
    depth = pieces_count * pieces[0].shape[2]
    row = lax.broadcasted_iota(jnp.int32, (depth, band), 0)
    col = lax.broadcasted_iota(jnp.int32, (depth, band), 1)
    inside = (row >= col + 1) & (row <= col + band)
    leading = row == col + 1
    r = lax.broadcasted_iota(jnp.int32, (band, band), 0)
    c = lax.broadcasted_iota(jnp.int32, (band, band), 1)
    slots = range(group)
    vs, ts, factors, inverses = [], [], [], []
    for g in slots:
        parts = [piece[0, g] for piece in pieces]
        stride = 1
        while stride < pieces_count:
            odd = (me // stride) % 2 == 1
            parts = [
                jnp.where(odd, parts[j ^ stride], parts[j]) for j in range(pieces_count)
            ]
            stride *= 2
        panel = jnp.concatenate(parts, axis=0)
        v = jnp.where(leading, 1.0, jnp.where(inside, panel, 0.0))
        vs.append(split(v))
        ts.append(split(v.T))
        vh_ref[g] = vs[g][0]
        vl_ref[g] = vs[g][1]
    for g in slots:
        gram = dot3(ts[g], vs[g])
        diagonal = jnp.sum(jnp.where(r == c, gram, 0.0), axis=0, keepdims=True)
        factors.append(gram)
        inverses.append(jnp.where(r == c, 2.0 / diagonal, 0.0))
    block = 1
    while block < band:
        coupling = (r // block != c // block) & (r // (2 * block) == c // (2 * block)) & (r < c)
        inverse_parts = [split(inverses[g]) for g in slots]
        middles = [
            split(dot3(split(jnp.where(coupling, factors[g], 0.0)), inverse_parts[g]))
            for g in slots
        ]
        inverses = [inverses[g] - dot3(inverse_parts[g], middles[g]) for g in slots]
        block *= 2
    for g in slots:
        high, low = split(dot3(split(inverses[g]), ts[g]))
        yh_ref[g] = high
        yl_ref[g] = low


def factor(slots, diagonal, col, pieces):
    count = len(pieces)
    _, _, height, band = pieces[0].shape
    depth = count * height
    group = GROUP if slots % GROUP == 0 else 1
    kind = jnp.bfloat16
    return pl.pallas_call(
        functools.partial(factor_kernel, count),
        grid_spec=pltpu.PrefetchScalarGridSpec(
            num_scalar_prefetch=1,
            grid=(slots // group,),
            in_specs=[
                pl.BlockSpec((1, group, height, band), lambda k, c: (diagonal, k, 0, 0))
            ] * count,
            out_specs=[pl.BlockSpec((group, depth, band), lambda k, c: (k, 0, 0))] * 2
            + [pl.BlockSpec((group, band, depth), lambda k, c: (k, 0, 0))] * 2,
        ),
        out_shape=[jax.ShapeDtypeStruct((slots, depth, band), kind)] * 2
        + [jax.ShapeDtypeStruct((slots, band, depth), kind)] * 2,
        name="factor",
    )(col, *pieces)


def apply_kernel(diagonal, own, counts, tile, below, vh, vl, yh, yl, tile_out, below_out):
    k = pl.program_id(0)
    band = tile.shape[1]
    upper, lower = tile[0], below[0]
    stacked = jnp.concatenate([upper, lower], axis=0)
    solved = dot3((yh[0], yl[0]), split(stacked))
    change = dot3((vh[0], vl[0]), split(solved))
    active = k < counts[0, diagonal]
    tile_out[0] = jnp.where(active, upper - change[:band], upper)
    below_out[0] = jnp.where(active, lower - change[band:], lower)


def apply(slots, diagonal, own, counts, tiles, beneath, vh, vl, yh, yl):
    _, band, columns = tiles.shape
    depth = vh.shape[1]
    at_slot = lambda k, own, counts: (k, 0, 0)
    at_own = lambda k, own, counts: (own[diagonal, k], 0, 0)
    return pl.pallas_call(
        functools.partial(apply_kernel, diagonal),
        grid_spec=pltpu.PrefetchScalarGridSpec(
            num_scalar_prefetch=2,
            grid=(slots,),
            in_specs=[
                pl.BlockSpec((1, band, columns), at_own),
                pl.BlockSpec((1, band, columns), at_slot),
                pl.BlockSpec((1, depth, band), at_slot),
                pl.BlockSpec((1, depth, band), at_slot),
                pl.BlockSpec((1, band, depth), at_slot),
                pl.BlockSpec((1, band, depth), at_slot),
            ],
            out_specs=[
                pl.BlockSpec((1, band, columns), at_own),
                pl.BlockSpec((1, band, columns), at_slot),
            ],
        ),
        out_shape=[
            jax.ShapeDtypeStruct(tiles.shape, tiles.dtype),
            jax.ShapeDtypeStruct(beneath.shape, beneath.dtype),
        ],
        input_output_aliases={2: 0},
        name="apply",
    )(own, counts, tiles, beneath, vh, vl, yh, yl)


def run(slots, own, behind, counts, tiles, panels):
    row_count = lax.axis_size("row")
    col_count = lax.axis_size("col")
    col = lax.axis_index("col").astype(jnp.int32)[None]
    diagonals = panels.shape[0]
    to_above = [(i, (i - 1) % row_count) for i in range(row_count)]
    to_below = [(i, (i + 1) % row_count) for i in range(row_count)]
    picked, sent = gather(slots, own, behind, panels, tiles)
    pieces = {0: picked}
    stride = col_count // 2
    while stride >= 1:
        swap = [(i, i ^ stride) for i in range(col_count)]
        pieces.update({q ^ stride: lax.ppermute(p, "col", swap) for q, p in pieces.items()})
        stride //= 2
    pieces = [pieces[q] for q in range(col_count)]
    for diagonal in range(diagonals):
        beneath = lax.ppermute(sent, "row", to_above)
        factors = factor(slots, diagonal, col, pieces)
        tiles, lower = apply(slots, diagonal, own, counts, tiles, beneath, *factors)
        returned = lax.ppermute(lower, "row", to_below)
        more = diagonal + 1 < diagonals
        result = scatter(slots, diagonal, more, behind, counts, tiles, returned)
        tiles = result[0]
        if more:
            sent = result[1]
    return tiles


def ordering(active):
    depth = active.shape[-1]
    here = jnp.arange(depth, dtype=jnp.int32)
    on = active.astype(jnp.int32)
    earlier = here[None, :] < here[:, None]
    before = jnp.sum(jnp.where(earlier, on[..., None, :], 0), axis=-1)
    total = jnp.sum(on, axis=-1)
    rank = jnp.where(active, before, total[..., None] + here - before)
    order = jnp.sum(
        jnp.where(rank[..., None, :] == here[:, None], here, 0), axis=-1
    ).astype(jnp.int32)
    return order, total.astype(jnp.int32)


def local(eigvec, reflectors, sweep_group):
    row_index = lax.axis_index("row")
    row_count = lax.axis_size("row")
    depth = eigvec.shape[0]
    active = lax.all_gather(sweep_group[:, :, 0], "row") >= 0
    most = jnp.max(jnp.sum(active.astype(jnp.int32), axis=-1))
    mine = lax.dynamic_index_in_dim(active, row_index, 0, keepdims=False)
    above = lax.dynamic_index_in_dim(
        active, (row_index + row_count - 1) % row_count, 0, keepdims=False
    )
    order, counts = ordering(jnp.stack([mine, above]))
    own = order[0]
    behind = jnp.where(row_index == 0, (order[1] + 1) % depth, order[1])
    sizes = [k for k in SLOT_SIZES if k < depth] + [depth]
    choice = sum((most > k).astype(jnp.int32) for k in sizes[:-1])
    branches = [functools.partial(run, k) for k in sizes]
    args = (own, behind, counts, eigvec[:, 0], reflectors[:, :, 0])
    if len(branches) == 1:
        out = branches[0](*args)
    else:
        out = lax.switch(choice, branches, *args)
    return out[:, None]


def solution(mesh):
    return jax.shard_map(
        local,
        mesh=mesh,
        in_specs=(
            P(None, "row", None, "col"),
            P(None, None, "row", "col", None),
            P(None, None, "row"),
        ),
        out_specs=P(None, "row", None, "col"),
        check_vma=False,
    )
```

```python
import functools

import jax
import jax.numpy as jnp
from jax import lax
from jax.experimental import pallas as pl
from jax.experimental.pallas import tpu as pltpu
from jax.sharding import PartitionSpec as P

SLOT_SIZES = (10, 12, 14, 16)
GROUP = 2
CHUNKS = 2


def split(x):
    high = x.astype(jnp.bfloat16)
    return high, (x - high.astype(jnp.float32)).astype(jnp.bfloat16)


def dot(a, b):
    return jnp.dot(a, b, preferred_element_type=jnp.float32)


def dot3(a, b):
    return dot(a[1], b[0]) + dot(a[0], b[1]) + dot(a[0], b[0])


def bounds(slots):
    return [slots * i // CHUNKS for i in range(CHUNKS + 1)]


def chunk_shapes(slots, tiles):
    edges = bounds(slots)
    return [
        jax.ShapeDtypeStruct((high - low,) + tiles.shape[1:], tiles.dtype)
        for low, high in zip(edges[:-1], edges[1:])
    ]


def slot_of(chunks, k):
    for chunk in chunks:
        if k < chunk.shape[0]:
            return chunk.at[k]
        k -= chunk.shape[0]


def gather_kernel(slots, own, behind, panels, tiles, picked, *rest):
    diagonals = panels.shape[0]
    sent, sems = rest[:-1], rest[-1]

    def panel_copy(d, k):
        return pltpu.make_async_copy(
            panels.at[d, own[d, k]], picked.at[d, k], sems.at[d * slots + k]
        )

    def tile_copy(k):
        return pltpu.make_async_copy(
            tiles.at[behind[0, k]], slot_of(sent, k), sems.at[diagonals * slots + k]
        )

    for k in range(slots):
        tile_copy(k).start()
    for d in range(diagonals):
        for k in range(slots):
            panel_copy(d, k).start()
    for k in range(slots):
        tile_copy(k).wait()
    for d in range(diagonals):
        for k in range(slots):
            panel_copy(d, k).wait()


def gather(slots, own, behind, panels, tiles):
    diagonals = panels.shape[0]
    any_spec = pl.BlockSpec(memory_space=pl.ANY)
    return pl.pallas_call(
        functools.partial(gather_kernel, slots),
        grid_spec=pltpu.PrefetchScalarGridSpec(
            num_scalar_prefetch=2,
            grid=(1,),
            in_specs=[any_spec, any_spec],
            out_specs=[pl.BlockSpec(memory_space=pltpu.VMEM)] * (1 + CHUNKS),
            scratch_shapes=[pltpu.SemaphoreType.DMA(((diagonals + 1) * slots,))],
        ),
        out_shape=[
            jax.ShapeDtypeStruct((diagonals, slots) + panels.shape[2:], panels.dtype),
        ] + chunk_shapes(slots, tiles),
        name="gather",
    )(own, behind, panels, tiles)


def scatter_kernel(slots, diagonal, more, behind, counts, tiles, *rest):
    returned, out, sent, sems = rest[:CHUNKS], rest[CHUNKS], rest[CHUNKS + 1:-1], rest[-1]

    def put(k):
        return pltpu.make_async_copy(
            slot_of(returned, k), out.at[behind[diagonal, k]], sems.at[k]
        )

    for k in range(slots):
        @pl.when(k < counts[1, diagonal])
        def _():
            put(k).start()
    for k in range(slots):
        @pl.when(k < counts[1, diagonal])
        def _():
            put(k).wait()
    if more:

        def take(k):
            return pltpu.make_async_copy(
                out.at[behind[diagonal + 1, k]], slot_of(sent, k), sems.at[slots + k]
            )

        for k in range(slots):
            take(k).start()
        for k in range(slots):
            take(k).wait()


def scatter(slots, diagonal, more, behind, counts, tiles, returned):
    any_spec = pl.BlockSpec(memory_space=pl.ANY)
    vmem_spec = pl.BlockSpec(memory_space=pltpu.VMEM)
    shapes = [jax.ShapeDtypeStruct(tiles.shape, tiles.dtype)]
    if more:
        shapes += chunk_shapes(slots, tiles)
    return pl.pallas_call(
        functools.partial(scatter_kernel, slots, diagonal, more),
        grid_spec=pltpu.PrefetchScalarGridSpec(
            num_scalar_prefetch=2,
            grid=(1,),
            in_specs=[any_spec] + [vmem_spec] * CHUNKS,
            out_specs=[any_spec] + [vmem_spec] * (len(shapes) - 1),
            scratch_shapes=[pltpu.SemaphoreType.DMA((2 * slots,))],
        ),
        out_shape=shapes,
        input_output_aliases={2: 0},
        name="scatter",
    )(behind, counts, tiles, *returned)


def factor_kernel(pieces_count, col_ref, *refs):
    pieces = refs[:pieces_count]
    vh_ref, vl_ref, yh_ref, yl_ref = refs[pieces_count:]
    me = col_ref[0]
    group = pieces[0].shape[1]
    band = pieces[0].shape[-1]
    depth = pieces_count * pieces[0].shape[2]
    row = lax.broadcasted_iota(jnp.int32, (depth, band), 0)
    col = lax.broadcasted_iota(jnp.int32, (depth, band), 1)
    inside = (row >= col + 1) & (row <= col + band)
    leading = row == col + 1
    r = lax.broadcasted_iota(jnp.int32, (band, band), 0)
    c = lax.broadcasted_iota(jnp.int32, (band, band), 1)
    slots = range(group)
    vs, ts, factors, inverses = [], [], [], []
    for g in slots:
        parts = [piece[0, g] for piece in pieces]
        stride = 1
        while stride < pieces_count:
            odd = (me // stride) % 2 == 1
            parts = [
                jnp.where(odd, parts[j ^ stride], parts[j]) for j in range(pieces_count)
            ]
            stride *= 2
        panel = jnp.concatenate(parts, axis=0)
        v = jnp.where(leading, 1.0, jnp.where(inside, panel, 0.0))
        vs.append(split(v))
        ts.append(split(v.T))
        vh_ref[g] = vs[g][0]
        vl_ref[g] = vs[g][1]
    for g in slots:
        gram = dot3(ts[g], vs[g])
        diagonal = jnp.sum(jnp.where(r == c, gram, 0.0), axis=0, keepdims=True)
        factors.append(gram)
        inverses.append(jnp.where(r == c, 2.0 / diagonal, 0.0))
    block = 1
    while block < band:
        coupling = (r // block != c // block) & (r // (2 * block) == c // (2 * block)) & (r < c)
        inverse_parts = [split(inverses[g]) for g in slots]
        middles = [
            split(dot3(split(jnp.where(coupling, factors[g], 0.0)), inverse_parts[g]))
            for g in slots
        ]
        inverses = [inverses[g] - dot3(inverse_parts[g], middles[g]) for g in slots]
        block *= 2
    for g in slots:
        high, low = split(dot3(split(inverses[g]), ts[g]))
        yh_ref[g] = high
        yl_ref[g] = low


def factor(slots, diagonal, col, pieces):
    count = len(pieces)
    _, _, height, band = pieces[0].shape
    depth = count * height
    group = GROUP if slots % GROUP == 0 else 1
    kind = jnp.bfloat16
    return pl.pallas_call(
        functools.partial(factor_kernel, count),
        grid_spec=pltpu.PrefetchScalarGridSpec(
            num_scalar_prefetch=1,
            grid=(slots // group,),
            in_specs=[
                pl.BlockSpec((1, group, height, band), lambda k, c: (diagonal, k, 0, 0))
            ] * count,
            out_specs=[pl.BlockSpec((group, depth, band), lambda k, c: (k, 0, 0))] * 2
            + [pl.BlockSpec((group, band, depth), lambda k, c: (k, 0, 0))] * 2,
        ),
        out_shape=[jax.ShapeDtypeStruct((slots, depth, band), kind)] * 2
        + [jax.ShapeDtypeStruct((slots, band, depth), kind)] * 2,
        name="factor",
    )(col, *pieces)


def apply_kernel(diagonal, first, own, counts, tile, below, vh, vl, yh, yl, tile_out, below_out):
    k = pl.program_id(0) + first
    band = tile.shape[1]
    upper, lower = tile[0], below[0]
    stacked = jnp.concatenate([upper, lower], axis=0)
    solved = dot3((yh[0], yl[0]), split(stacked))
    change = dot3((vh[0], vl[0]), split(solved))
    active = k < counts[0, diagonal]
    tile_out[0] = jnp.where(active, upper - change[:band], upper)
    below_out[0] = jnp.where(active, lower - change[band:], lower)


def apply(first, diagonal, own, counts, tiles, beneath, vh, vl, yh, yl):
    _, band, columns = tiles.shape
    depth = vh.shape[1]
    at_slot = lambda k, own, counts: (k, 0, 0)
    at_factor = lambda k, own, counts: (k + first, 0, 0)
    at_own = lambda k, own, counts: (own[diagonal, k + first], 0, 0)
    return pl.pallas_call(
        functools.partial(apply_kernel, diagonal, first),
        grid_spec=pltpu.PrefetchScalarGridSpec(
            num_scalar_prefetch=2,
            grid=(beneath.shape[0],),
            in_specs=[
                pl.BlockSpec((1, band, columns), at_own),
                pl.BlockSpec((1, band, columns), at_slot),
                pl.BlockSpec((1, depth, band), at_factor),
                pl.BlockSpec((1, depth, band), at_factor),
                pl.BlockSpec((1, band, depth), at_factor),
                pl.BlockSpec((1, band, depth), at_factor),
            ],
            out_specs=[
                pl.BlockSpec((1, band, columns), at_own),
                pl.BlockSpec((1, band, columns), at_slot),
            ],
        ),
        out_shape=[
            jax.ShapeDtypeStruct(tiles.shape, tiles.dtype),
            jax.ShapeDtypeStruct(beneath.shape, beneath.dtype),
        ],
        input_output_aliases={2: 0},
        name="apply",
    )(own, counts, tiles, beneath, vh, vl, yh, yl)


def run(slots, own, behind, counts, tiles, panels):
    row_count = lax.axis_size("row")
    col_count = lax.axis_size("col")
    col = lax.axis_index("col").astype(jnp.int32)[None]
    diagonals = panels.shape[0]
    to_above = [(i, (i - 1) % row_count) for i in range(row_count)]
    to_below = [(i, (i + 1) % row_count) for i in range(row_count)]
    picked, *sent = gather(slots, own, behind, panels, tiles)
    pieces = {0: picked}
    stride = col_count // 2
    while stride >= 1:
        swap = [(i, i ^ stride) for i in range(col_count)]
        pieces.update({q ^ stride: lax.ppermute(p, "col", swap) for q, p in pieces.items()})
        stride //= 2
    pieces = [pieces[q] for q in range(col_count)]
    for diagonal in range(diagonals):
        beneath = [lax.ppermute(chunk, "row", to_above) for chunk in sent]
        factors = factor(slots, diagonal, col, pieces)
        returned = []
        for first, chunk in zip(bounds(slots), beneath):
            tiles, lower = apply(first, diagonal, own, counts, tiles, chunk, *factors)
            returned.append(lax.ppermute(lower, "row", to_below))
        more = diagonal + 1 < diagonals
        tiles, *sent = scatter(slots, diagonal, more, behind, counts, tiles, returned)
    return tiles


def share_kernel(flags, out, held, send, recv):
    count = held.shape[0]
    me = lax.axis_index("row")
    barrier = pltpu.get_barrier_semaphore()
    mesh_id = pl.DeviceIdType.MESH
    others = [lax.rem(me + by, count) for by in range(1, count)]
    for other in others:
        pl.semaphore_signal(
            barrier, inc=1, device_id={"row": other}, device_id_type=mesh_id
        )
    pl.semaphore_wait(barrier, count - 1)
    copies = [
        pltpu.make_async_remote_copy(
            src_ref=flags,
            dst_ref=held.at[me],
            send_sem=send.at[i],
            recv_sem=recv.at[i],
            device_id={"row": other},
            device_id_type=mesh_id,
        )
        for i, other in enumerate(others)
    ]
    for copy in copies:
        copy.start()
    held[me] = flags[...]
    for copy in copies:
        copy.wait()
    out[...] = held[...]


def share(flags):
    count = lax.axis_size("row")
    diagonals, depth = flags.shape
    rows, lanes = -(-diagonals // 8) * 8, -(-depth // 128) * 128
    padded = jnp.pad(flags, ((0, rows - diagonals), (0, lanes - depth)))
    vmem_spec = pl.BlockSpec(memory_space=pltpu.VMEM)
    shape = (count, rows, lanes)
    gathered = pl.pallas_call(
        share_kernel,
        out_shape=jax.ShapeDtypeStruct(shape, flags.dtype),
        in_specs=[vmem_spec],
        out_specs=vmem_spec,
        scratch_shapes=[
            pltpu.VMEM(shape, flags.dtype),
            pltpu.SemaphoreType.DMA((count - 1,)),
            pltpu.SemaphoreType.DMA((count - 1,)),
        ],
        compiler_params=pltpu.CompilerParams(collective_id=0, has_side_effects=True),
        name="share",
    )(padded)
    return gathered[:, :diagonals, :depth]


def ordering(active):
    depth = active.shape[-1]
    here = jnp.arange(depth, dtype=jnp.int32)
    on = active.astype(jnp.int32)
    earlier = here[None, :] < here[:, None]
    before = jnp.sum(jnp.where(earlier, on[..., None, :], 0), axis=-1)
    total = jnp.sum(on, axis=-1)
    rank = jnp.where(active, before, total[..., None] + here - before)
    order = jnp.sum(
        jnp.where(rank[..., None, :] == here[:, None], here, 0), axis=-1
    ).astype(jnp.int32)
    return order, total.astype(jnp.int32)


def local(eigvec, reflectors, sweep_group):
    row_index = lax.axis_index("row")
    row_count = lax.axis_size("row")
    depth = eigvec.shape[0]
    active = share(sweep_group[:, :, 0]) >= 0
    most = jnp.max(jnp.sum(active.astype(jnp.int32), axis=-1))
    mine = lax.dynamic_index_in_dim(active, row_index, 0, keepdims=False)
    above = lax.dynamic_index_in_dim(
        active, (row_index + row_count - 1) % row_count, 0, keepdims=False
    )
    order, counts = ordering(jnp.stack([mine, above]))
    own = order[0]
    behind = jnp.where(row_index == 0, (order[1] + 1) % depth, order[1])
    sizes = [k for k in SLOT_SIZES if k < depth] + [depth]
    choice = sum((most > k).astype(jnp.int32) for k in sizes[:-1])
    branches = [functools.partial(run, k) for k in sizes]
    args = (own, behind, counts, eigvec[:, 0], reflectors[:, :, 0])
    if len(branches) == 1:
        out = branches[0](*args)
    else:
        out = lax.switch(choice, branches, *args)
    return out[:, None]


def solution(mesh):
    return jax.shard_map(
        local,
        mesh=mesh,
        in_specs=(
            P(None, "row", None, "col"),
            P(None, None, "row", "col", None),
            P(None, None, "row"),
        ),
        out_specs=P(None, "row", None, "col"),
        check_vma=False,
    )
```

```python
import functools

import jax
import jax.numpy as jnp
from jax import lax
from jax.experimental import pallas as pl
from jax.experimental.pallas import tpu as pltpu
from jax.sharding import PartitionSpec as P


SLOT_SIZES = (10, 12, 14, 16)
GROUP = 2
CHUNKS = 2


def split(x):
    high = x.astype(jnp.bfloat16)
    return high, (x - high.astype(jnp.float32)).astype(jnp.bfloat16)


def dot(a, b):
    return jnp.dot(a, b, preferred_element_type=jnp.float32)


def dot3(a, b):
    return dot(a[1], b[0]) + dot(a[0], b[1]) + dot(a[0], b[0])


def bounds(slots):
    return [slots * i // CHUNKS for i in range(CHUNKS + 1)]


def chunk_shapes(slots, tiles):
    edges = bounds(slots)
    return [
        jax.ShapeDtypeStruct((high - low,) + tiles.shape[1:], tiles.dtype)
        for low, high in zip(edges[:-1], edges[1:])
    ]


def slot_of(chunks, k):
    for chunk in chunks:
        if k < chunk.shape[0]:
            return chunk.at[k]
        k -= chunk.shape[0]


def gather_kernel(slots, own, behind, panels, tiles, picked, *rest):
    diagonals = panels.shape[0]
    sent, sems = rest[:-1], rest[-1]

    def panel_copy(d, k):
        return pltpu.make_async_copy(
            panels.at[d, own[d, k]], picked.at[d, k], sems.at[d * slots + k]
        )

    def tile_copy(k):
        return pltpu.make_async_copy(
            tiles.at[behind[0, k]], slot_of(sent, k), sems.at[diagonals * slots + k]
        )

    for k in range(slots):
        tile_copy(k).start()
    for d in range(diagonals):
        for k in range(slots):
            panel_copy(d, k).start()
    for k in range(slots):
        tile_copy(k).wait()
    for d in range(diagonals):
        for k in range(slots):
            panel_copy(d, k).wait()


def gather(slots, own, behind, panels, tiles):
    diagonals = panels.shape[0]
    any_spec = pl.BlockSpec(memory_space=pl.ANY)
    return pl.pallas_call(
        functools.partial(gather_kernel, slots),
        grid_spec=pltpu.PrefetchScalarGridSpec(
            num_scalar_prefetch=2,
            grid=(1,),
            in_specs=[any_spec, any_spec],
            out_specs=[pl.BlockSpec(memory_space=pltpu.VMEM)] * (1 + CHUNKS),
            scratch_shapes=[pltpu.SemaphoreType.DMA(((diagonals + 1) * slots,))],
        ),
        out_shape=[
            jax.ShapeDtypeStruct((diagonals, slots) + panels.shape[2:], panels.dtype),
        ] + chunk_shapes(slots, tiles),
        name="gather",
    )(own, behind, panels, tiles)


def scatter_kernel(slots, diagonal, more, behind, counts, tiles, *rest):
    returned, out, sent, sems = rest[:CHUNKS], rest[CHUNKS], rest[CHUNKS + 1:-1], rest[-1]

    def put(k):
        return pltpu.make_async_copy(
            slot_of(returned, k), out.at[behind[diagonal, k]], sems.at[k]
        )

    for k in range(slots):
        @pl.when(k < counts[1, diagonal])
        def _():
            put(k).start()
    for k in range(slots):
        @pl.when(k < counts[1, diagonal])
        def _():
            put(k).wait()
    if more:

        def take(k):
            return pltpu.make_async_copy(
                out.at[behind[diagonal + 1, k]], slot_of(sent, k), sems.at[slots + k]
            )

        for k in range(slots):
            take(k).start()
        for k in range(slots):
            take(k).wait()


def scatter(slots, diagonal, more, behind, counts, tiles, returned):
    any_spec = pl.BlockSpec(memory_space=pl.ANY)
    vmem_spec = pl.BlockSpec(memory_space=pltpu.VMEM)
    shapes = [jax.ShapeDtypeStruct(tiles.shape, tiles.dtype)]
    if more:
        shapes += chunk_shapes(slots, tiles)
    return pl.pallas_call(
        functools.partial(scatter_kernel, slots, diagonal, more),
        grid_spec=pltpu.PrefetchScalarGridSpec(
            num_scalar_prefetch=2,
            grid=(1,),
            in_specs=[any_spec] + [vmem_spec] * CHUNKS,
            out_specs=[any_spec] + [vmem_spec] * (len(shapes) - 1),
            scratch_shapes=[pltpu.SemaphoreType.DMA((2 * slots,))],
        ),
        out_shape=shapes,
        input_output_aliases={2: 0},
        name="scatter",
    )(behind, counts, tiles, *returned)


def factor_kernel(pieces_count, col_ref, *refs):
    pieces = refs[:pieces_count]
    vh_ref, vl_ref, yh_ref, yl_ref = refs[pieces_count:]
    me = col_ref[0]
    group = pieces[0].shape[1]
    band = pieces[0].shape[-1]
    depth = pieces_count * pieces[0].shape[2]
    row = lax.broadcasted_iota(jnp.int32, (depth, band), 0)
    col = lax.broadcasted_iota(jnp.int32, (depth, band), 1)
    inside = (row >= col + 1) & (row <= col + band)
    leading = row == col + 1
    r = lax.broadcasted_iota(jnp.int32, (band, band), 0)
    c = lax.broadcasted_iota(jnp.int32, (band, band), 1)
    slots = range(group)
    vs, ts, factors, inverses = [], [], [], []
    for g in slots:
        parts = [piece[0, g] for piece in pieces]
        stride = 1
        while stride < pieces_count:
            odd = (me // stride) % 2 == 1
            parts = [
                jnp.where(odd, parts[j ^ stride], parts[j]) for j in range(pieces_count)
            ]
            stride *= 2
        panel = jnp.concatenate(parts, axis=0)
        v = jnp.where(leading, 1.0, jnp.where(inside, panel, 0.0))
        vs.append(split(v))
        ts.append(split(v.T))
        vh_ref[g] = vs[g][0]
        vl_ref[g] = vs[g][1]
    for g in slots:
        gram = dot3(ts[g], vs[g])
        diagonal = jnp.sum(jnp.where(r == c, gram, 0.0), axis=0, keepdims=True)
        factors.append(gram)
        inverses.append(jnp.where(r == c, 2.0 / diagonal, 0.0))
    block = 1
    while block < band:
        coupling = (r // block != c // block) & (r // (2 * block) == c // (2 * block)) & (r < c)
        inverse_parts = [split(inverses[g]) for g in slots]
        middles = [
            split(dot3(split(jnp.where(coupling, factors[g], 0.0)), inverse_parts[g]))
            for g in slots
        ]
        inverses = [inverses[g] - dot3(inverse_parts[g], middles[g]) for g in slots]
        block *= 2
    for g in slots:
        high, low = split(dot3(split(inverses[g]), ts[g]))
        yh_ref[g] = high
        yl_ref[g] = low


def factor(slots, diagonal, col, pieces):
    count = len(pieces)
    _, _, height, band = pieces[0].shape
    depth = count * height
    group = GROUP if slots % GROUP == 0 else 1
    kind = jnp.bfloat16
    return pl.pallas_call(
        functools.partial(factor_kernel, count),
        grid_spec=pltpu.PrefetchScalarGridSpec(
            num_scalar_prefetch=1,
            grid=(slots // group,),
            in_specs=[
                pl.BlockSpec((1, group, height, band), lambda k, c: (diagonal, k, 0, 0))
            ] * count,
            out_specs=[pl.BlockSpec((group, depth, band), lambda k, c: (k, 0, 0))] * 2
            + [pl.BlockSpec((group, band, depth), lambda k, c: (k, 0, 0))] * 2,
        ),
        out_shape=[jax.ShapeDtypeStruct((slots, depth, band), kind)] * 2
        + [jax.ShapeDtypeStruct((slots, band, depth), kind)] * 2,
        name="factor",
    )(col, *pieces)


def apply_kernel(diagonal, first, own, counts, tile, below, vh, vl, yh, yl, tile_out, below_out):
    k = pl.program_id(0) + first
    band = tile.shape[1]
    upper, lower = tile[0], below[0]
    stacked = jnp.concatenate([upper, lower], axis=0)
    solved = dot3((yh[0], yl[0]), split(stacked))
    change = dot3((vh[0], vl[0]), split(solved))
    active = k < counts[0, diagonal]
    tile_out[0] = jnp.where(active, upper - change[:band], upper)
    below_out[0] = jnp.where(active, lower - change[band:], lower)


def apply(first, diagonal, own, counts, tiles, beneath, vh, vl, yh, yl):
    _, band, columns = tiles.shape
    depth = vh.shape[1]
    at_slot = lambda k, own, counts: (k, 0, 0)
    at_factor = lambda k, own, counts: (k + first, 0, 0)
    at_own = lambda k, own, counts: (own[diagonal, k + first], 0, 0)
    return pl.pallas_call(
        functools.partial(apply_kernel, diagonal, first),
        grid_spec=pltpu.PrefetchScalarGridSpec(
            num_scalar_prefetch=2,
            grid=(beneath.shape[0],),
            in_specs=[
                pl.BlockSpec((1, band, columns), at_own),
                pl.BlockSpec((1, band, columns), at_slot),
                pl.BlockSpec((1, depth, band), at_factor),
                pl.BlockSpec((1, depth, band), at_factor),
                pl.BlockSpec((1, band, depth), at_factor),
                pl.BlockSpec((1, band, depth), at_factor),
            ],
            out_specs=[
                pl.BlockSpec((1, band, columns), at_own),
                pl.BlockSpec((1, band, columns), at_slot),
            ],
        ),
        out_shape=[
            jax.ShapeDtypeStruct(tiles.shape, tiles.dtype),
            jax.ShapeDtypeStruct(beneath.shape, beneath.dtype),
        ],
        input_output_aliases={2: 0},
        name="apply",
    )(own, counts, tiles, beneath, vh, vl, yh, yl)


def lift(sent, to_above):
    beneath = []
    for chunk in sent:
        beneath.append(lax.ppermute(chunk, "row", to_above))
    return beneath


def run(slots, *args):
    return steps(slots, *args)


def steps(slots, own, behind, counts, tiles, panels):
    row_count = lax.axis_size("row")
    col_count = lax.axis_size("col")
    col = lax.axis_index("col").astype(jnp.int32)[None]
    diagonals = panels.shape[0]
    to_above = [(i, (i - 1) % row_count) for i in range(row_count)]
    to_below = [(i, (i + 1) % row_count) for i in range(row_count)]
    picked, *sent = gather(slots, own, behind, panels, tiles)
    beneath = lift(sent, to_above)
    pieces = {0: picked}
    stride = col_count // 2
    while stride >= 1:
        swap = [(i, i ^ stride) for i in range(col_count)]
        pieces.update(
            {q ^ stride: lax.ppermute(p, "col", swap) for q, p in pieces.items()}
        )
        stride //= 2
    pieces = [pieces[q] for q in range(col_count)]
    for diagonal in range(diagonals):
        factors = factor(slots, diagonal, col, pieces)
        returned = []
        for first, chunk in zip(bounds(slots), beneath):
            tiles, lower = apply(first, diagonal, own, counts, tiles, chunk, *factors)
            returned.append(lax.ppermute(lower, "row", to_below))
        more = diagonal + 1 < diagonals
        tiles, *sent = scatter(slots, diagonal, more, behind, counts, tiles, returned)
        if more:
            beneath = lift(sent, to_above)
    return tiles


def share_kernel(flags, out, held, send, recv):
    count = held.shape[0]
    me = lax.axis_index("row")
    barrier = pltpu.get_barrier_semaphore()
    mesh_id = pl.DeviceIdType.MESH
    others = [lax.rem(me + by, count) for by in range(1, count)]
    for other in others:
        pl.semaphore_signal(
            barrier, inc=1, device_id={"row": other}, device_id_type=mesh_id
        )
    pl.semaphore_wait(barrier, count - 1)
    copies = [
        pltpu.make_async_remote_copy(
            src_ref=flags,
            dst_ref=held.at[me],
            send_sem=send.at[i],
            recv_sem=recv.at[i],
            device_id={"row": other},
            device_id_type=mesh_id,
        )
        for i, other in enumerate(others)
    ]
    for copy in copies:
        copy.start()
    held[me] = flags[...]
    for copy in copies:
        copy.wait()
    out[...] = held[...]


def share(flags):
    count = lax.axis_size("row")
    diagonals, depth = flags.shape
    rows, lanes = -(-diagonals // 8) * 8, -(-depth // 128) * 128
    padded = jnp.pad(flags, ((0, rows - diagonals), (0, lanes - depth)))
    vmem_spec = pl.BlockSpec(memory_space=pltpu.VMEM)
    shape = (count, rows, lanes)
    gathered = pl.pallas_call(
        share_kernel,
        out_shape=jax.ShapeDtypeStruct(shape, flags.dtype),
        in_specs=[vmem_spec],
        out_specs=vmem_spec,
        scratch_shapes=[
            pltpu.VMEM(shape, flags.dtype),
            pltpu.SemaphoreType.DMA((count - 1,)),
            pltpu.SemaphoreType.DMA((count - 1,)),
        ],
        compiler_params=pltpu.CompilerParams(collective_id=0, has_side_effects=True),
        name="share",
    )(padded)
    return gathered[:, :diagonals, :depth]


def ordering(active):
    depth = active.shape[-1]
    here = jnp.arange(depth, dtype=jnp.int32)
    on = active.astype(jnp.int32)
    earlier = here[None, :] < here[:, None]
    before = jnp.sum(jnp.where(earlier, on[..., None, :], 0), axis=-1)
    total = jnp.sum(on, axis=-1)
    rank = jnp.where(active, before, total[..., None] + here - before)
    order = jnp.sum(
        jnp.where(rank[..., None, :] == here[:, None], here, 0), axis=-1
    ).astype(jnp.int32)
    return order, total.astype(jnp.int32)


def local(eigvec, reflectors, sweep_group):
    row_index = lax.axis_index("row")
    row_count = lax.axis_size("row")
    depth = eigvec.shape[0]
    active = share(sweep_group[:, :, 0]) >= 0
    most = jnp.max(jnp.sum(active.astype(jnp.int32), axis=-1))
    mine = lax.dynamic_index_in_dim(active, row_index, 0, keepdims=False)
    above = lax.dynamic_index_in_dim(
        active, (row_index + row_count - 1) % row_count, 0, keepdims=False
    )
    order, counts = ordering(jnp.stack([mine, above]))
    own = order[0]
    behind = jnp.where(row_index == 0, (order[1] + 1) % depth, order[1])
    sizes = [k for k in SLOT_SIZES if k < depth] + [depth]
    choice = sum((most > k).astype(jnp.int32) for k in sizes[:-1])
    branches = [functools.partial(run, k) for k in sizes]
    args = (own, behind, counts, eigvec[:, 0], reflectors[:, :, 0])
    if len(branches) == 1:
        out = branches[0](*args)
    else:
        out = lax.switch(choice, branches, *args)
    return out[:, None]


def solution(mesh):
    return jax.shard_map(
        local,
        mesh=mesh,
        in_specs=(
            P(None, "row", None, "col"),
            P(None, None, "row", "col", None),
            P(None, None, "row"),
        ),
        out_specs=P(None, "row", None, "col"),
        check_vma=False,
    )
```

```python
import functools

import jax
import jax.numpy as jnp
from jax import lax
from jax.experimental import pallas as pl
from jax.experimental.pallas import tpu as pltpu
from jax.sharding import PartitionSpec as P


SLOT_SIZES = (12, 14, 16)
GROUP = 2
CHUNKS = 2


def split(x):
    high = x.astype(jnp.bfloat16)
    return high, (x - high.astype(jnp.float32)).astype(jnp.bfloat16)


def dot(a, b):
    return jnp.dot(a, b, preferred_element_type=jnp.float32)


def dot3(a, b):
    return dot(a[1], b[0]) + dot(a[0], b[1]) + dot(a[0], b[0])


def bounds(slots):
    inner = [slots * i // CHUNKS // GROUP * GROUP for i in range(CHUNKS)]
    return inner + [slots]


def chunk_shapes(slots, tiles):
    edges = bounds(slots)
    return [
        jax.ShapeDtypeStruct((high - low,) + tiles.shape[1:], tiles.dtype)
        for low, high in zip(edges[:-1], edges[1:])
    ]


def slot_of(chunks, k):
    for chunk in chunks:
        if k < chunk.shape[0]:
            return chunk.at[k]
        k -= chunk.shape[0]


def gather_kernel(slots, own, behind, panels, tiles, picked, *rest):
    diagonals = panels.shape[0]
    sent, sems = rest[:-1], rest[-1]

    def panel_copy(d, k):
        return pltpu.make_async_copy(
            panels.at[d, own[d, k]], picked.at[d, k], sems.at[d * slots + k]
        )

    def tile_copy(k):
        return pltpu.make_async_copy(
            tiles.at[behind[0, k]], slot_of(sent, k), sems.at[diagonals * slots + k]
        )

    for k in range(slots):
        tile_copy(k).start()
    for d in range(diagonals):
        for k in range(slots):
            panel_copy(d, k).start()
    for k in range(slots):
        tile_copy(k).wait()
    for d in range(diagonals):
        for k in range(slots):
            panel_copy(d, k).wait()


def gather(slots, own, behind, panels, tiles):
    diagonals = panels.shape[0]
    any_spec = pl.BlockSpec(memory_space=pl.ANY)
    return pl.pallas_call(
        functools.partial(gather_kernel, slots),
        grid_spec=pltpu.PrefetchScalarGridSpec(
            num_scalar_prefetch=2,
            grid=(1,),
            in_specs=[any_spec, any_spec],
            out_specs=[pl.BlockSpec(memory_space=pltpu.VMEM)] * (1 + CHUNKS),
            scratch_shapes=[pltpu.SemaphoreType.DMA(((diagonals + 1) * slots,))],
        ),
        out_shape=[
            jax.ShapeDtypeStruct((diagonals, slots) + panels.shape[2:], panels.dtype),
        ] + chunk_shapes(slots, tiles),
        name="gather",
    )(own, behind, panels, tiles)


def scatter_kernel(slots, diagonal, more, behind, counts, tiles, *rest):
    returned, out, sent, sems = rest[:CHUNKS], rest[CHUNKS], rest[CHUNKS + 1:-1], rest[-1]

    def put(k):
        return pltpu.make_async_copy(
            slot_of(returned, k), out.at[behind[diagonal, k]], sems.at[k]
        )

    for k in range(slots):
        @pl.when(k < counts[1, diagonal])
        def _():
            put(k).start()
    for k in range(slots):
        @pl.when(k < counts[1, diagonal])
        def _():
            put(k).wait()
    if more:

        def take(k):
            return pltpu.make_async_copy(
                out.at[behind[diagonal + 1, k]], slot_of(sent, k), sems.at[slots + k]
            )

        for k in range(slots):
            take(k).start()
        for k in range(slots):
            take(k).wait()


def scatter(slots, diagonal, more, behind, counts, tiles, returned):
    any_spec = pl.BlockSpec(memory_space=pl.ANY)
    vmem_spec = pl.BlockSpec(memory_space=pltpu.VMEM)
    shapes = [jax.ShapeDtypeStruct(tiles.shape, tiles.dtype)]
    if more:
        shapes += chunk_shapes(slots, tiles)
    return pl.pallas_call(
        functools.partial(scatter_kernel, slots, diagonal, more),
        grid_spec=pltpu.PrefetchScalarGridSpec(
            num_scalar_prefetch=2,
            grid=(1,),
            in_specs=[any_spec] + [vmem_spec] * CHUNKS,
            out_specs=[any_spec] + [vmem_spec] * (len(shapes) - 1),
            scratch_shapes=[pltpu.SemaphoreType.DMA((2 * slots,))],
        ),
        out_shape=shapes,
        input_output_aliases={2: 0},
        name="scatter",
    )(behind, counts, tiles, *returned)


def factor_kernel(pieces_count, col_ref, *refs):
    pieces = refs[:pieces_count]
    vh_ref, vl_ref, yh_ref, yl_ref = refs[pieces_count:]
    me = col_ref[0]
    group = pieces[0].shape[1]
    band = pieces[0].shape[-1]
    depth = pieces_count * pieces[0].shape[2]
    row = lax.broadcasted_iota(jnp.int32, (depth, band), 0)
    col = lax.broadcasted_iota(jnp.int32, (depth, band), 1)
    inside = (row >= col + 1) & (row <= col + band)
    leading = row == col + 1
    r = lax.broadcasted_iota(jnp.int32, (band, band), 0)
    c = lax.broadcasted_iota(jnp.int32, (band, band), 1)
    slots = range(group)
    vs, ts, factors, inverses = [], [], [], []
    for g in slots:
        parts = [piece[0, g] for piece in pieces]
        stride = 1
        while stride < pieces_count:
            odd = (me // stride) % 2 == 1
            parts = [
                jnp.where(odd, parts[j ^ stride], parts[j]) for j in range(pieces_count)
            ]
            stride *= 2
        panel = jnp.concatenate(parts, axis=0)
        v = jnp.where(leading, 1.0, jnp.where(inside, panel, 0.0))
        vs.append(split(v))
        ts.append(split(v.T))
        vh_ref[g] = vs[g][0]
        vl_ref[g] = vs[g][1]
    for g in slots:
        gram = dot3(ts[g], vs[g])
        diagonal = jnp.sum(jnp.where(r == c, gram, 0.0), axis=0, keepdims=True)
        factors.append(gram)
        inverses.append(jnp.where(r == c, 2.0 / diagonal, 0.0))

    def level(n, inverses):
        coupling = ((r >> n) != (c >> n)) & ((r >> (n + 1)) == (c >> (n + 1))) & (r < c)
        inverse_parts = [split(inverse) for inverse in inverses]
        middles = [
            split(dot3(split(jnp.where(coupling, factors[g], 0.0)), inverse_parts[g]))
            for g in slots
        ]
        return tuple(inverses[g] - dot3(inverse_parts[g], middles[g]) for g in slots)

    inverses = lax.fori_loop(0, (band - 1).bit_length(), level, tuple(inverses))
    for g in slots:
        high, low = split(dot3(split(inverses[g]), ts[g]))
        yh_ref[g] = high
        yl_ref[g] = low


def factor(first, slots, diagonal, col, pieces):
    count = len(pieces)
    _, _, height, band = pieces[0].shape
    depth = count * height
    group = GROUP if slots % GROUP == 0 else 1
    start = first // group
    kind = jnp.bfloat16
    return pl.pallas_call(
        functools.partial(factor_kernel, count),
        grid_spec=pltpu.PrefetchScalarGridSpec(
            num_scalar_prefetch=1,
            grid=(slots // group,),
            in_specs=[
                pl.BlockSpec((1, group, height, band), lambda k, c: (diagonal, k + start, 0, 0))
            ] * count,
            out_specs=[pl.BlockSpec((group, depth, band), lambda k, c: (k, 0, 0))] * 2
            + [pl.BlockSpec((group, band, depth), lambda k, c: (k, 0, 0))] * 2,
        ),
        out_shape=[jax.ShapeDtypeStruct((slots, depth, band), kind)] * 2
        + [jax.ShapeDtypeStruct((slots, band, depth), kind)] * 2,
        name="factor",
    )(col, *pieces)


def apply_kernel(diagonal, first, own, counts, tile, below, vh, vl, yh, yl, tile_out, below_out):
    k = pl.program_id(0) + first
    band = tile.shape[1]
    upper, lower = tile[0], below[0]
    stacked = jnp.concatenate([upper, lower], axis=0)
    solved = dot3((yh[0], yl[0]), split(stacked))
    change = dot3((vh[0], vl[0]), split(solved))
    active = k < counts[0, diagonal]
    tile_out[0] = jnp.where(active, upper - change[:band], upper)
    below_out[0] = jnp.where(active, lower - change[band:], lower)


def apply(first, diagonal, own, counts, tiles, beneath, vh, vl, yh, yl):
    _, band, columns = tiles.shape
    depth = vh.shape[1]
    at_slot = lambda k, own, counts: (k, 0, 0)
    at_own = lambda k, own, counts: (own[diagonal, k + first], 0, 0)
    return pl.pallas_call(
        functools.partial(apply_kernel, diagonal, first),
        grid_spec=pltpu.PrefetchScalarGridSpec(
            num_scalar_prefetch=2,
            grid=(beneath.shape[0],),
            in_specs=[
                pl.BlockSpec((1, band, columns), at_own),
                pl.BlockSpec((1, band, columns), at_slot),
                pl.BlockSpec((1, depth, band), at_slot),
                pl.BlockSpec((1, depth, band), at_slot),
                pl.BlockSpec((1, band, depth), at_slot),
                pl.BlockSpec((1, band, depth), at_slot),
            ],
            out_specs=[
                pl.BlockSpec((1, band, columns), at_own),
                pl.BlockSpec((1, band, columns), at_slot),
            ],
        ),
        out_shape=[
            jax.ShapeDtypeStruct(tiles.shape, tiles.dtype),
            jax.ShapeDtypeStruct(beneath.shape, beneath.dtype),
        ],
        input_output_aliases={2: 0},
        name="apply",
    )(own, counts, tiles, beneath, vh, vl, yh, yl)


def lift(sent, to_above):
    beneath = []
    for chunk in sent:
        beneath.append(lax.ppermute(chunk, "row", to_above))
    return beneath


def run(slots, *args):
    return steps(slots, *args)


def steps(slots, own, behind, counts, tiles, panels):
    row_count = lax.axis_size("row")
    col_count = lax.axis_size("col")
    col = lax.axis_index("col").astype(jnp.int32)[None]
    diagonals = panels.shape[0]
    to_above = [(i, (i - 1) % row_count) for i in range(row_count)]
    to_below = [(i, (i + 1) % row_count) for i in range(row_count)]
    picked, *sent = gather(slots, own, behind, panels, tiles)
    beneath = lift(sent, to_above)
    pieces = {0: picked}
    stride = col_count // 2
    while stride >= 1:
        swap = [(i, i ^ stride) for i in range(col_count)]
        pieces.update(
            {q ^ stride: lax.ppermute(p, "col", swap) for q, p in pieces.items()}
        )
        stride //= 2
    pieces = [pieces[q] for q in range(col_count)]
    for diagonal in range(diagonals):
        returned = []
        for first, chunk in zip(bounds(slots), beneath):
            factors = factor(first, chunk.shape[0], diagonal, col, pieces)
            tiles, lower = apply(first, diagonal, own, counts, tiles, chunk, *factors)
            returned.append(lax.ppermute(lower, "row", to_below))
        more = diagonal + 1 < diagonals
        tiles, *sent = scatter(slots, diagonal, more, behind, counts, tiles, returned)
        if more:
            beneath = lift(sent, to_above)
    return tiles


def share_kernel(flags, out, held, send, recv):
    count = held.shape[0]
    me = lax.axis_index("row")
    barrier = pltpu.get_barrier_semaphore()
    mesh_id = pl.DeviceIdType.MESH
    others = [lax.rem(me + by, count) for by in range(1, count)]
    for other in others:
        pl.semaphore_signal(
            barrier, inc=1, device_id={"row": other}, device_id_type=mesh_id
        )
    pl.semaphore_wait(barrier, count - 1)
    copies = [
        pltpu.make_async_remote_copy(
            src_ref=flags,
            dst_ref=held.at[me],
            send_sem=send.at[i],
            recv_sem=recv.at[i],
            device_id={"row": other},
            device_id_type=mesh_id,
        )
        for i, other in enumerate(others)
    ]
    for copy in copies:
        copy.start()
    held[me] = flags[...]
    for copy in copies:
        copy.wait()
    out[...] = held[...]


def share(flags):
    count = lax.axis_size("row")
    diagonals, depth = flags.shape
    rows, lanes = -(-diagonals // 8) * 8, -(-depth // 128) * 128
    padded = jnp.pad(flags, ((0, rows - diagonals), (0, lanes - depth)))
    vmem_spec = pl.BlockSpec(memory_space=pltpu.VMEM)
    shape = (count, rows, lanes)
    gathered = pl.pallas_call(
        share_kernel,
        out_shape=jax.ShapeDtypeStruct(shape, flags.dtype),
        in_specs=[vmem_spec],
        out_specs=vmem_spec,
        scratch_shapes=[
            pltpu.VMEM(shape, flags.dtype),
            pltpu.SemaphoreType.DMA((count - 1,)),
            pltpu.SemaphoreType.DMA((count - 1,)),
        ],
        compiler_params=pltpu.CompilerParams(collective_id=0, has_side_effects=True),
        name="share",
    )(padded)
    return gathered[:, :diagonals, :depth]


def ordering(active):
    depth = active.shape[-1]
    here = jnp.arange(depth, dtype=jnp.int32)
    on = active.astype(jnp.int32)
    earlier = here[None, :] < here[:, None]
    before = jnp.sum(jnp.where(earlier, on[..., None, :], 0), axis=-1)
    total = jnp.sum(on, axis=-1)
    rank = jnp.where(active, before, total[..., None] + here - before)
    order = jnp.sum(
        jnp.where(rank[..., None, :] == here[:, None], here, 0), axis=-1
    ).astype(jnp.int32)
    return order, total.astype(jnp.int32)


def local(eigvec, reflectors, sweep_group):
    row_index = lax.axis_index("row")
    row_count = lax.axis_size("row")
    depth = eigvec.shape[0]
    active = share(sweep_group[:, :, 0]) >= 0
    most = jnp.max(jnp.sum(active.astype(jnp.int32), axis=-1))
    mine = lax.dynamic_index_in_dim(active, row_index, 0, keepdims=False)
    above = lax.dynamic_index_in_dim(
        active, (row_index + row_count - 1) % row_count, 0, keepdims=False
    )
    order, counts = ordering(jnp.stack([mine, above]))
    own = order[0]
    behind = jnp.where(row_index == 0, (order[1] + 1) % depth, order[1])
    sizes = [k for k in SLOT_SIZES if k < depth] + [depth]
    choice = sum((most > k).astype(jnp.int32) for k in sizes[:-1])
    branches = [functools.partial(run, k) for k in sizes]
    args = (own, behind, counts, eigvec[:, 0], reflectors[:, :, 0])
    if len(branches) == 1:
        out = branches[0](*args)
    else:
        out = lax.switch(choice, branches, *args)
    return out[:, None]


def solution(mesh):
    return jax.shard_map(
        local,
        mesh=mesh,
        in_specs=(
            P(None, "row", None, "col"),
            P(None, None, "row", "col", None),
            P(None, None, "row"),
        ),
        out_specs=P(None, "row", None, "col"),
        check_vma=False,
    )
```
